32 devices in a mesh: gx: 4 (over y, x), gy: 2 (over core), gz: 4 (over z).
Axes of the slice: x: 2, y: 2, z: 4, core: 2. Of those that a mesh axis runs over, the one named last changes fastest.
Arguments:
- gradient: bfloat16 [32, 32, 16, 512], P(None, 'gx', 'gy', 'gz'), may hold values from -6 to 6
- noise_draw: bfloat16 [32, 32, 16, 512], P(None, 'gx', 'gy', 'gz'), may hold values from -6 to 6
- current: float32 [32, 32, 16, 512], P(None, 'gx', 'gy', 'gz'), may hold values from -6 to 6
- eigvectors: bfloat16 [32, 16, 512, 512], P('gx', 'gy', 'gz'), may hold values from -0.125 to 0.125
- eigvalues: float32 [512], replicated, may hold values from 0.05 to 50
- reaction: float32 [32, 16, 512], P('gx', 'gy', 'gz'), may hold values from 0.25 to 4
Outputs:
- proposal: float32 [32, 32, 16, 512], P(None, 'gx', 'gy', 'gz')
The draws below stay inside these ranges and needn't reach their ends.
All inputs are finite; a program needn't handle non-finite values.
Results may differ from the reference program's by a relative error of at most 0.00031.
Values sent between devices are 32-bit elements; how exact they have to be, the bound alone decides.
A program may use at most 64 MiB of HBM per device.

```python
import math
import jax
import jax.numpy as jnp
from jax import lax

R = 512
CHAINS = 32
SWEEPS = 4
NX = 32
NY = 16
NZ = 512


def block_scale(stream_key, dims, cuts, least, largest):
    loudness, own = 1.0, jax.random.fold_in(stream_key, 6)
    for dim, parts in cuts:
        heights = jnp.exp(jax.random.uniform(jax.random.fold_in(own, dim), (parts,), jnp.float32, least / len(cuts), largest / len(cuts)))
        loudness = loudness * jnp.repeat(heights, dims[dim] // parts).reshape([-1 if axis == dim else 1 for axis in range(len(dims))])
    return loudness


def normal_values(rng, shape, spread, reach, cuts=(), kind=jnp.bfloat16):
    entries = jax.random.normal(rng, shape, jnp.float32) * spread
    if len(cuts) > 0:
        entries = block_scale(rng, shape, cuts, -0.22, 0.18) * entries
    return jnp.clip(entries, min=-reach, max=reach).astype(kind)


def setup_inputs(seed: int = 0) -> dict:
    streams_of = jax.random.split(jax.random.key(seed), 7)
    gradient = normal_values(streams_of[0], (CHAINS, NX, NY, NZ), 1.0, 6.0, ((1, 4), (2, 2), (3, 4)))
    noise_draw = normal_values(streams_of[1], (CHAINS, NX, NY, NZ), 1.0, 6.0, ((1, 4), (2, 2), (3, 4)))
    current = normal_values(streams_of[2], (CHAINS, NX, NY, NZ), 1.0, 6.0, ((1, 4), (2, 2), (3, 4)), jnp.float32)
    eigvectors = normal_values(streams_of[3], (NX, NY, NZ, R), ((R * NX * NY * NZ) ** -0.25), 0.125, ((0, 4), (1, 2), (2, 4)))
    eigvalues = jnp.clip(jnp.exp(jax.random.uniform(streams_of[4], (R,), jnp.float32, math.log(0.05), math.log(50.0))), 0.05, 50.0)
    reaction = jnp.clip(jnp.exp(math.log(4.0) - 2.7725887 * jax.random.uniform(streams_of[5], (NX, NY, NZ), jnp.float32) ** block_scale(streams_of[5], (NX, NY, NZ), ((0, 4), (1, 2), (2, 4)), -0.2, 0.2)), 0.25, 4.0)
    return dict(gradient=gradient, noise_draw=noise_draw, current=current, eigvectors=eigvectors, eigvalues=eigvalues, reaction=reaction)


def neighbours(field):
    padded = jnp.pad(field, ((0, 0), (1, 1), (1, 1), (1, 1)))
    total = padded[:, 2:, 1:-1, 1:-1] + padded[:, :-2, 1:-1, 1:-1]
    total = total + padded[:, 1:-1, 2:, 1:-1] + padded[:, 1:-1, :-2, 1:-1]
    total = total + padded[:, 1:-1, 1:-1, 2:] + padded[:, 1:-1, 1:-1, :-2]
    return total

def reference(gradient, noise_draw, current, eigvectors, eigvalues, reaction):
    stacked = jnp.concatenate([gradient, noise_draw], 0)
    slabs = jnp.moveaxis(stacked, 1, 0)

    def accumulate(total, pair):
        basis_slab, data_slab = pair
        rows = basis_slab.reshape(-1, R)
        vectors = data_slab.reshape(data_slab.shape[0], -1)
        return (total + jnp.dot(vectors, rows, preferred_element_type=jnp.float32), None)
    start = jnp.zeros((2 * CHAINS, R), jnp.float32)
    sums, _ = lax.scan(accumulate, start, (eigvectors, slabs))
    proj_grad = sums[:CHAINS]
    proj_noise = sums[CHAINS:]
    damp = eigvalues / (eigvalues + 1.0)
    root_damp = 1.0 - 1.0 / jnp.sqrt(1.0 + eigvalues)
    coef = (0.5 * damp * proj_grad - 1.0 * root_damp * proj_noise).astype(jnp.bfloat16)

    def expand(basis_slab):
        rows = basis_slab.reshape(-1, R)
        return lax.dot_general(coef, rows, (((1,), (1,)), ((), ())), preferred_element_type=jnp.float32)
    corr_slabs = lax.map(expand, eigvectors)
    corr = jnp.moveaxis(corr_slabs, 0, 1).reshape(current.shape)
    source = -0.5 * gradient.astype(jnp.float32) + 1.0 * noise_draw.astype(jnp.float32) + corr
    diagonal = reaction + 6.0
    field = source / diagonal
    for sweep_index in range(SWEEPS - 1):
        field = (source + neighbours(field)) / diagonal
    return current + field
```

```python
import functools

import jax
import jax.numpy as jnp
from jax import lax
from jax.experimental import pallas as pl
from jax.experimental.pallas import tpu as pltpu
from jax.sharding import PartitionSpec as P

SWEEPS = 4
GROUPS = 4
MESH = pl.DeviceIdType.MESH
AXES = ("gx", "gy", "gz")


def kernel(
    sizes, shape, g_h, n_h, cur_h, eig_h, ev_ref, rea_h, out_h,
    eig_v, gb, nb, gf, nf, cur_v, rdv, lhs, src, fields, zout, zin,
    part, got1, got2, full, load_sem, out_sem,
    send1, recv1, send2, recv2, send3, recv3, hsend, hrecv,
):
    C, X, Y, Z, R = shape
    NX, NY, NZ = sizes
    G = src.shape[0]
    CG = C // G
    XY = X * Y
    S = SWEEPS - 1
    PL = NX * NY
    rows = part.shape[1]
    pos = {a: lax.axis_index(a) for a in AXES}
    count = dict(zip(AXES, sizes))
    me_p = pos["gx"] * NY + pos["gy"]
    me_z = pos["gz"]

    loads = [
        pltpu.make_async_copy(g_h, gb, load_sem.at[0]),
        pltpu.make_async_copy(n_h, nb, load_sem.at[1]),
        pltpu.make_async_copy(rea_h, rdv, load_sem.at[2]),
        pltpu.make_async_copy(cur_h, cur_v, load_sem.at[3]),
    ]
    eig_loads = [
        pltpu.make_async_copy(eig_h.at[x], eig_v.at[x], load_sem.at[4 + x]) for x in range(X)
    ]
    for c in loads[:3] + eig_loads + loads[3:]:
        c.start()

    barrier = pltpu.get_barrier_semaphore()

    def plane_peer(d):
        q = lax.rem(me_p + d, PL)
        return {"gx": q // NY, "gy": lax.rem(q, NY)}, q

    for d in range(1, PL):
        pl.semaphore_signal(barrier, inc=1, device_id=plane_peer(d)[0], device_id_type=MESH)
    for d in range(1, NZ):
        pl.semaphore_signal(
            barrier, inc=1, device_id={"gz": lax.rem(me_z + d, NZ)}, device_id_type=MESH
        )

    zeros = jnp.zeros((Y, CG, Z), jnp.float32)
    zerosy = jnp.zeros((X, CG, Z), jnp.float32)

    def fill(cond, fn):
        if cond is True:
            fn()
        else:
            pl.when(cond)(fn)

    def low_edge(a):
        return True if count[a] == 1 else pos[a] == 0

    def high_edge(a):
        return True if count[a] == 1 else pos[a] == count[a] - 1

    for k in range(S):
        for g in range(G):
            def x0(k=k, g=g):
                fields[k, g, 0, 1 : Y + 1] = zeros
            def x1(k=k, g=g):
                fields[k, g, X + 1, 1 : Y + 1] = zeros
            def y0(k=k, g=g):
                fields[k, g, 1 : X + 1, 0] = zerosy
            def y1(k=k, g=g):
                fields[k, g, 1 : X + 1, Y + 1] = zerosy
            def z0(k=k, g=g):
                zin[k, g, 0] = jnp.zeros((CG, Z), jnp.float32)
            def z1(k=k, g=g):
                zin[k, g, 1] = jnp.zeros((CG, Z), jnp.float32)
            fill(low_edge("gx"), x0)
            fill(high_edge("gx"), x1)
            fill(low_edge("gy"), y0)
            fill(high_edge("gy"), y1)
            fill(low_edge("gz"), z0)
            fill(high_edge("gz"), z1)

    loads[0].wait()
    loads[1].wait()
    loads[2].wait()
    rdv[...] = 1.0 / (rdv[...] + 6.0)
    CH = XY
    @pl.loop(0, C)
    def _(c):
        r = pl.ds(pl.multiple_of(c * CH, CH), CH)
        gf[r, :] = gb[r, :].astype(jnp.float32)
        nf[r, :] = nb[r, :].astype(jnp.float32)

    @pl.loop(0, X)
    def _(x):
        for y in range(Y):
            at = pl.ds(x * Y + y, C, stride=XY)
            gv = gf[at, :]
            nv = nf[at, :]
            lhs[x, 0:C, y * Z : (y + 1) * Z] = gv.astype(jnp.bfloat16)
            lhs[x, C : 2 * C, y * Z : (y + 1) * Z] = nv.astype(jnp.bfloat16)
            s = -0.5 * gv + nv
            for g in range(G):
                src[g, x, y] = s[g * CG : (g + 1) * CG]

    acc = None
    for x in range(X):
        eig_loads[x].wait()
        term = jnp.dot(lhs[x], eig_v[x], preferred_element_type=jnp.float32)
        acc = term if acc is None else acc + term
    ev = ev_ref[...]
    damp = ev / (ev + 1.0)
    root_damp = 1.0 - 1.0 / jnp.sqrt(1.0 + ev)
    comb = (0.5 * damp) * acc[:C] - root_damp * acc[C:]
    RT = R // 128
    tiles = [(c, r) for c in range(C // 8) for r in range(RT)]
    for t, (c, r) in enumerate(tiles):
        tile = comb[c * 8 : (c + 1) * 8, r * 128 : (r + 1) * 128]
        if rows >= 8:
            o = (t * 8) % rows
            part[(t * 8) // rows, o : o + 8, :] = tile
        else:
            for j in range(8 // rows):
                part[(t * 8) // rows + j] = tile[j * rows : (j + 1) * rows]

    pl.semaphore_wait(barrier, PL - 1 + NZ - 1)

    copies1 = []
    for d in range(1, PL):
        dev, q = plane_peer(d)
        copies1.append(pltpu.make_async_remote_copy(
            src_ref=part.at[q], dst_ref=got1.at[d],
            send_sem=send1.at[d], recv_sem=recv1.at[d],
            device_id=dev, device_id_type=MESH))
    for c in copies1:
        c.start()
    total = part[me_p]
    for d in range(1, PL):
        copies1[d - 1].wait_recv()
        total = total + got1[d]
    got2[me_z] = total
    copies2 = []
    for d in range(1, NZ):
        copies2.append(pltpu.make_async_remote_copy(
            src_ref=got2.at[me_z], dst_ref=got2.at[me_z],
            send_sem=send2.at[d], recv_sem=recv2.at[d],
            device_id={"gz": lax.rem(me_z + d, NZ)}, device_id_type=MESH))
    for c in copies2:
        c.start()
    for c in copies2:
        c.wait_recv()
    total = got2[0]
    for j in range(1, NZ):
        total = total + got2[j]
    full[me_p] = total
    copies3 = []
    for d in range(1, PL):
        copies3.append(pltpu.make_async_remote_copy(
            src_ref=full.at[me_p], dst_ref=full.at[me_p],
            send_sem=send3.at[d], recv_sem=recv3.at[d],
            device_id=plane_peer(d)[0], device_id_type=MESH))
    for c in copies3:
        c.start()
    for c in copies3:
        c.wait_recv()
    bands = []
    for c in range(C // 8):
        band = []
        for r in range(RT):
            t = c * RT + r
            if rows >= 8:
                o = (t * 8) % rows
                band.append(full[(t * 8) // rows, o : o + 8, :])
            else:
                band.append(jnp.concatenate(
                    [full[(t * 8) // rows + j] for j in range(8 // rows)], 0))
        bands.append(jnp.concatenate(band, 1))
    coef = jnp.concatenate(bands, 0).astype(jnp.bfloat16)

    lane = lax.broadcasted_iota(jnp.int32, (CG, Z), 1)

    def halo(k, g, axis, sign):
        i = AXES.index(axis) * 2 + (sign > 0)
        if axis == "gx":
            s = fields.at[k, g, X if sign > 0 else 1, 1 : Y + 1]
            d = fields.at[k, g, 0 if sign > 0 else X + 1, 1 : Y + 1]
        elif axis == "gy":
            s = fields.at[k, g, 1 : X + 1, Y if sign > 0 else 1]
            d = fields.at[k, g, 1 : X + 1, 0 if sign > 0 else Y + 1]
        else:
            s = zout.at[k, g, 1 if sign > 0 else 0]
            d = zin.at[k, g, 0 if sign > 0 else 1]
        n = count[axis]
        to = lax.rem(pos[axis] + (sign + n), n)
        copy = pltpu.make_async_remote_copy(
            src_ref=s, dst_ref=d, send_sem=hsend.at[k, g, i], recv_sem=hrecv.at[k, g, i],
            device_id={axis: to}, device_id_type=MESH)
        up, down = pos[axis] < n - 1, pos[axis] > 0
        return copy, (up if sign > 0 else down), (down if sign > 0 else up)

    ways = [(a, s) for a in AXES if count[a] > 1 for s in (-1, 1)]

    def send(k, g, axes):
        for a, s in ways:
            if a in axes:
                copy, out, _ = halo(k, g, a, s)
                pl.when(out)(copy.start)

    def wait_halos(k, g):
        for a, s in ways:
            copy, _, come = halo(k, g, a, s)
            pl.when(come)(copy.wait_recv)

    def wait_sends(k, g):
        for a, s in ways:
            copy, out, _ = halo(k, g, a, s)
            pl.when(out)(copy.wait_send)

    def packed(x, y, f, low, high):
        l = x * Y + y
        low = jnp.where(lane == l, pltpu.roll(f, l, 1), low)
        high = jnp.where(lane == l, pltpu.roll(f, l + 1, 1), high)
        return low, high

    nothing = jnp.zeros((CG, Z), jnp.float32)

    def first(x, carry):
        corr = lax.dot_general(
            coef, eig_v[x], (((1,), (1,)), ((), ())), preferred_element_type=jnp.float32)
        rdx = rdv[x]
        carry = list(carry)
        for y in range(Y):
            for g in range(G):
                s = src[g, x, y] + corr[g * CG : (g + 1) * CG, y * Z : (y + 1) * Z]
                src[g, x, y] = s
                f = s * rdx[y : y + 1]
                fields[0, g, x + 1, y + 1] = f
                carry[2 * g], carry[2 * g + 1] = packed(x, y, f, carry[2 * g], carry[2 * g + 1])
        return tuple(carry)

    carry = first(0, (nothing,) * (2 * G))
    carry = first(X - 1, carry)
    for g in range(G):
        send(0, g, ("gx",))
    carry = lax.fori_loop(1, X - 1, first, carry)
    for g in range(G):
        zout[0, g, 0] = carry[2 * g]
        zout[0, g, 1] = carry[2 * g + 1]
    for g in range(G):
        send(0, g, ("gz", "gy"))

    loads[3].wait()
    outs = []
    for k in range(S):
        for g in range(G):
            wait_halos(k, g)
            zlo = zin[k, g, 0]
            zhi = zin[k, g, 1]

            def step(x, carry, k=k, g=g, zlo=zlo, zhi=zhi):
                rdx = rdv[x]
                low, high = carry
                for y in range(Y):
                    l = x * Y + y
                    f = fields[k, g, x + 1, y + 1]
                    t = fields[k, g, x + 2, y + 1] + fields[k, g, x, y + 1]
                    t = t + (fields[k, g, x + 1, y + 2] + fields[k, g, x + 1, y])
                    up = jnp.where(lane == Z - 1, pltpu.roll(zhi, Z - 1 - l, 1), pltpu.roll(f, Z - 1, 1))
                    down = jnp.where(lane == 0, pltpu.roll(zlo, lax.rem(Z - l, Z), 1), pltpu.roll(f, 1, 1))
                    v = (src[g, x, y] + (t + (up + down))) * rdx[y : y + 1]
                    if k < S - 1:
                        fields[k + 1, g, x + 1, y + 1] = v
                        low, high = packed(x, y, v, low, high)
                    else:
                        at = pl.ds(g * CG * XY + l, CG, stride=XY)
                        cur_v[at, :] = cur_v[at, :] + v
                return low, high

            low, high = lax.fori_loop(0, X, step, (nothing, nothing))
            if k < S - 1:
                zout[k + 1, g, 0] = low
                zout[k + 1, g, 1] = high
                send(k + 1, g, AXES)
            else:
                r = pl.ds(g * CG * XY, CG * XY)
                c = pltpu.make_async_copy(cur_v.at[r], out_h.at[r], out_sem.at[g])
                c.start()
                outs.append(c)
    for c in copies1 + copies2 + copies3:
        c.wait_send()
    for k in range(S):
        for g in range(G):
            wait_sends(k, g)
    for c in outs:
        c.wait()


def body(sizes, gradient, noise_draw, current, eigvectors, eigvalues, reaction):
    C, X, Y, Z = gradient.shape
    R = eigvectors.shape[3]
    NX, NY, NZ = sizes
    PL = NX * NY
    G = GROUPS
    CG = C // G
    S = SWEEPS - 1
    XY = X * Y
    f32, bf16 = jnp.float32, jnp.bfloat16
    rows = C * R // 128 // PL
    any_space = pl.BlockSpec(memory_space=pl.ANY)
    dma = pltpu.SemaphoreType.DMA
    out = pl.pallas_call(
        functools.partial(kernel, sizes, (C, X, Y, Z, R)),
        out_shape=jax.ShapeDtypeStruct((C * XY, Z), f32),
        in_specs=[any_space] * 4 + [pl.BlockSpec(memory_space=pltpu.VMEM), any_space],
        out_specs=any_space,
        scratch_shapes=[
            pltpu.VMEM((X, Y * Z, R), bf16),
            pltpu.VMEM((C * XY, Z), bf16),
            pltpu.VMEM((C * XY, Z), bf16),
            pltpu.VMEM((C * XY, Z), f32),
            pltpu.VMEM((C * XY, Z), f32),
            pltpu.VMEM((C * XY, Z), f32),
            pltpu.VMEM((X, Y, Z), f32),
            pltpu.VMEM((X, 2 * C, Y * Z), bf16),
            pltpu.VMEM((G, X, Y, CG, Z), f32),
            pltpu.VMEM((S, G, X + 2, Y + 2, CG, Z), f32),
            pltpu.VMEM((S, G, 2, CG, Z), f32),
            pltpu.VMEM((S, G, 2, CG, Z), f32),
            pltpu.VMEM((PL, rows, 128), f32),
            pltpu.VMEM((PL, rows, 128), f32),
            pltpu.VMEM((NZ, rows, 128), f32),
            pltpu.VMEM((PL, rows, 128), f32),
            dma((4 + X,)),
            dma((G,)),
            dma((PL,)), dma((PL,)),
            dma((NZ,)), dma((NZ,)),
            dma((PL,)), dma((PL,)),
            dma((S, G, 6)), dma((S, G, 6)),
        ],
        compiler_params=pltpu.CompilerParams(
            collective_id=0, has_side_effects=True, vmem_limit_bytes=48 * 1024 * 1024
        ),
    )(
        gradient.reshape(C * XY, Z),
        noise_draw.reshape(C * XY, Z),
        current.reshape(C * XY, Z),
        eigvectors.reshape(X, Y * Z, R),
        eigvalues.reshape(1, R),
        reaction,
    )
    return out.reshape(current.shape)


def solution(mesh):
    return jax.shard_map(
        functools.partial(body, tuple(mesh.shape[a] for a in AXES)),
        mesh=mesh,
        in_specs=(
            P(None, "gx", "gy", "gz"),
            P(None, "gx", "gy", "gz"),
            P(None, "gx", "gy", "gz"),
            P("gx", "gy", "gz", None),
            P(),
            P("gx", "gy", "gz"),
        ),
        out_specs=P(None, "gx", "gy", "gz"),
        check_vma=False,
    )
```

```python
import functools

import jax
import jax.numpy as jnp
from jax import lax
from jax.experimental import pallas as pl
from jax.experimental.pallas import tpu as pltpu
from jax.sharding import PartitionSpec as P

SWEEPS = 4
GROUPS = 2
MESH = pl.DeviceIdType.MESH
AXES = ("gx", "gy", "gz")


def kernel(
    sizes, shape, g_h, n_h, cur_h, eig_h, ev_ref, rea_h, out_h,
    eig_v, gb, nb, gf, nf, cur_v, rdv, lhs, src, fields, zout, zin,
    part, got1, got2, full, load_sem, out_sem,
    send1, recv1, send2, recv2, send3, recv3, hsend, hrecv,
):
    C, X, Y, Z, R = shape
    NX, NY, NZ = sizes
    G = src.shape[0]
    CG = C // G
    XY = X * Y
    S = SWEEPS - 1
    PL = NX * NY
    rows = part.shape[1]
    pos = {a: lax.axis_index(a) for a in AXES}
    count = dict(zip(AXES, sizes))
    me_p = pos["gx"] * NY + pos["gy"]
    me_z = pos["gz"]

    loads = [
        pltpu.make_async_copy(g_h, gb, load_sem.at[0]),
        pltpu.make_async_copy(n_h, nb, load_sem.at[1]),
        pltpu.make_async_copy(rea_h, rdv, load_sem.at[2]),
        pltpu.make_async_copy(cur_h, cur_v, load_sem.at[3]),
    ]
    eig_loads = [
        pltpu.make_async_copy(eig_h.at[x], eig_v.at[x], load_sem.at[4 + x]) for x in range(X)
    ]
    for c in loads[:3] + eig_loads + loads[3:]:
        c.start()

    barrier = pltpu.get_barrier_semaphore()

    def plane_peer(d):
        q = lax.rem(me_p + d, PL)
        return {"gx": q // NY, "gy": lax.rem(q, NY)}, q

    for d in range(1, PL):
        pl.semaphore_signal(barrier, inc=1, device_id=plane_peer(d)[0], device_id_type=MESH)
    for d in range(1, NZ):
        pl.semaphore_signal(
            barrier, inc=1, device_id={"gz": lax.rem(me_z + d, NZ)}, device_id_type=MESH
        )

    zeros = jnp.zeros((Y, CG, Z), jnp.float32)
    zerosy = jnp.zeros((X, CG, Z), jnp.float32)

    def fill(cond, fn):
        if cond is True:
            fn()
        else:
            pl.when(cond)(fn)

    def low_edge(a):
        return True if count[a] == 1 else pos[a] == 0

    def high_edge(a):
        return True if count[a] == 1 else pos[a] == count[a] - 1

    for k in range(S):
        for g in range(G):
            def x0(k=k, g=g):
                fields[k, g, 0, 1 : Y + 1] = zeros
            def x1(k=k, g=g):
                fields[k, g, X + 1, 1 : Y + 1] = zeros
            def y0(k=k, g=g):
                fields[k, g, 1 : X + 1, 0] = zerosy
            def y1(k=k, g=g):
                fields[k, g, 1 : X + 1, Y + 1] = zerosy
            def z0(k=k, g=g):
                zin[k, g, 0] = jnp.zeros((CG, Z), jnp.float32)
            def z1(k=k, g=g):
                zin[k, g, 1] = jnp.zeros((CG, Z), jnp.float32)
            fill(low_edge("gx"), x0)
            fill(high_edge("gx"), x1)
            fill(low_edge("gy"), y0)
            fill(high_edge("gy"), y1)
            fill(low_edge("gz"), z0)
            fill(high_edge("gz"), z1)

    loads[0].wait()
    loads[1].wait()
    loads[2].wait()
    rdv[...] = 1.0 / (rdv[...] + 6.0)
    CH = XY
    @pl.loop(0, C)
    def _(c):
        r = pl.ds(pl.multiple_of(c * CH, CH), CH)
        gf[r, :] = gb[r, :].astype(jnp.float32)
        nf[r, :] = nb[r, :].astype(jnp.float32)

    @pl.loop(0, X)
    def _(x):
        for y in range(Y):
            at = pl.ds(x * Y + y, C, stride=XY)
            gv = gf[at, :]
            nv = nf[at, :]
            lhs[x, 0:C, y * Z : (y + 1) * Z] = gv.astype(jnp.bfloat16)
            lhs[x, C : 2 * C, y * Z : (y + 1) * Z] = nv.astype(jnp.bfloat16)
            s = -0.5 * gv + nv
            for g in range(G):
                src[g, x, y] = s[g * CG : (g + 1) * CG]

    acc = None
    for x in range(X):
        eig_loads[x].wait()
        term = jnp.dot(lhs[x], eig_v[x], preferred_element_type=jnp.float32)
        acc = term if acc is None else acc + term
    ev = ev_ref[...]
    damp = ev / (ev + 1.0)
    root_damp = 1.0 - 1.0 / jnp.sqrt(1.0 + ev)
    comb = (0.5 * damp) * acc[:C] - root_damp * acc[C:]
    RT = R // 128
    tiles = [(c, r) for c in range(C // 8) for r in range(RT)]
    for t, (c, r) in enumerate(tiles):
        tile = comb[c * 8 : (c + 1) * 8, r * 128 : (r + 1) * 128]
        if rows >= 8:
            o = (t * 8) % rows
            part[(t * 8) // rows, o : o + 8, :] = tile
        else:
            for j in range(8 // rows):
                part[(t * 8) // rows + j] = tile[j * rows : (j + 1) * rows]

    pl.semaphore_wait(barrier, PL - 1 + NZ - 1)

    copies1 = []
    for d in range(1, PL):
        dev, q = plane_peer(d)
        copies1.append(pltpu.make_async_remote_copy(
            src_ref=part.at[q], dst_ref=got1.at[d],
            send_sem=send1.at[d], recv_sem=recv1.at[d],
            device_id=dev, device_id_type=MESH))
    for c in copies1:
        c.start()
    total = part[me_p]
    for d in range(1, PL):
        copies1[d - 1].wait_recv()
        total = total + got1[d]
    got2[me_z] = total
    copies2 = []
    for d in range(1, NZ):
        copies2.append(pltpu.make_async_remote_copy(
            src_ref=got2.at[me_z], dst_ref=got2.at[me_z],
            send_sem=send2.at[d], recv_sem=recv2.at[d],
            device_id={"gz": lax.rem(me_z + d, NZ)}, device_id_type=MESH))
    for c in copies2:
        c.start()
    for c in copies2:
        c.wait_recv()
    total = got2[0]
    for j in range(1, NZ):
        total = total + got2[j]
    full[me_p] = total
    copies3 = []
    for d in range(1, PL):
        copies3.append(pltpu.make_async_remote_copy(
            src_ref=full.at[me_p], dst_ref=full.at[me_p],
            send_sem=send3.at[d], recv_sem=recv3.at[d],
            device_id=plane_peer(d)[0], device_id_type=MESH))
    for c in copies3:
        c.start()
    for c in copies3:
        c.wait_recv()
    bands = []
    for c in range(C // 8):
        band = []
        for r in range(RT):
            t = c * RT + r
            if rows >= 8:
                o = (t * 8) % rows
                band.append(full[(t * 8) // rows, o : o + 8, :])
            else:
                band.append(jnp.concatenate(
                    [full[(t * 8) // rows + j] for j in range(8 // rows)], 0))
        bands.append(jnp.concatenate(band, 1))
    coef = jnp.concatenate(bands, 0).astype(jnp.bfloat16)

    lane = lax.broadcasted_iota(jnp.int32, (CG, Z), 1)

    def halo(k, g, axis, sign):
        i = AXES.index(axis) * 2 + (sign > 0)
        if axis == "gx":
            s = fields.at[k, g, X if sign > 0 else 1, 1 : Y + 1]
            d = fields.at[k, g, 0 if sign > 0 else X + 1, 1 : Y + 1]
        elif axis == "gy":
            s = fields.at[k, g, 1 : X + 1, Y if sign > 0 else 1]
            d = fields.at[k, g, 1 : X + 1, 0 if sign > 0 else Y + 1]
        else:
            s = zout.at[k, g, 1 if sign > 0 else 0]
            d = zin.at[k, g, 0 if sign > 0 else 1]
        n = count[axis]
        to = lax.rem(pos[axis] + (sign + n), n)
        copy = pltpu.make_async_remote_copy(
            src_ref=s, dst_ref=d, send_sem=hsend.at[k, g, i], recv_sem=hrecv.at[k, g, i],
            device_id={axis: to}, device_id_type=MESH)
        up, down = pos[axis] < n - 1, pos[axis] > 0
        return copy, (up if sign > 0 else down), (down if sign > 0 else up)

    ways = [(a, s) for a in AXES if count[a] > 1 for s in (-1, 1)]

    def send(k, g, axes):
        for a, s in ways:
            if a in axes:
                copy, out, _ = halo(k, g, a, s)
                pl.when(out)(copy.start)

    def wait_halos(k, g):
        for a, s in ways:
            copy, _, come = halo(k, g, a, s)
            pl.when(come)(copy.wait_recv)

    def wait_sends(k, g):
        for a, s in ways:
            copy, out, _ = halo(k, g, a, s)
            pl.when(out)(copy.wait_send)

    def packed(x, y, f, low, high):
        l = x * Y + y
        low = jnp.where(lane == l, pltpu.roll(f, l, 1), low)
        high = jnp.where(lane == l, pltpu.roll(f, l + 1, 1), high)
        return low, high

    nothing = jnp.zeros((CG, Z), jnp.float32)

    def first(x, carry):
        corr = lax.dot_general(
            coef, eig_v[x], (((1,), (1,)), ((), ())), preferred_element_type=jnp.float32)
        rdx = rdv[x]
        carry = list(carry)
        for y in range(Y):
            for g in range(G):
                s = src[g, x, y] + corr[g * CG : (g + 1) * CG, y * Z : (y + 1) * Z]
                src[g, x, y] = s
                f = s * rdx[y : y + 1]
                fields[0, g, x + 1, y + 1] = f
                carry[2 * g], carry[2 * g + 1] = packed(x, y, f, carry[2 * g], carry[2 * g + 1])
        return tuple(carry)

    carry = first(0, (nothing,) * (2 * G))
    carry = first(X - 1, carry)
    for g in range(G):
        send(0, g, ("gx",))
    carry = lax.fori_loop(1, X - 1, first, carry)
    for g in range(G):
        zout[0, g, 0] = carry[2 * g]
        zout[0, g, 1] = carry[2 * g + 1]
    for g in range(G):
        send(0, g, ("gz", "gy"))

    loads[3].wait()
    outs = []
    for k in range(S):
        for g in range(G):
            wait_halos(k, g)
            zlo = zin[k, g, 0]
            zhi = zin[k, g, 1]

            def step(x, carry, k=k, g=g):
                rdx = rdv[x]
                low, high, zlo, zhi = carry
                low = pltpu.roll(low, Z - Y, 1)
                high = pltpu.roll(high, Z - Y, 1)
                done = []
                for y in range(Y):
                    f = fields[k, g, x + 1, y + 1]
                    t = fields[k, g, x + 2, y + 1] + fields[k, g, x, y + 1]
                    t = t + (fields[k, g, x + 1, y + 2] + fields[k, g, x + 1, y])
                    up = jnp.where(lane == Z - 1, pltpu.roll(zhi, Z - 1 - y, 1), pltpu.roll(f, Z - 1, 1))
                    down = jnp.where(lane == 0, pltpu.roll(zlo, (Z - y) % Z, 1), pltpu.roll(f, 1, 1))
                    v = (src[g, x, y] + (t + (up + down))) * rdx[y : y + 1]
                    if k < S - 1:
                        m = (X - 1) * Y + y
                        low = jnp.where(lane == m, pltpu.roll(v, m, 1), low)
                        high = jnp.where(lane == m, pltpu.roll(v, m + 1, 1), high)
                    else:
                        v = v + cur_v[pl.ds(g * CG * XY + x * Y + y, CG, stride=XY), :]
                    done.append(v)
                for y, v in enumerate(done):
                    if k < S - 1:
                        fields[k + 1, g, x + 1, y + 1] = v
                    else:
                        cur_v[pl.ds(g * CG * XY + x * Y + y, CG, stride=XY), :] = v
                return low, high, pltpu.roll(zlo, Z - Y, 1), pltpu.roll(zhi, Z - Y, 1)

            low, high, _, _ = lax.fori_loop(0, X, step, (nothing, nothing, zlo, zhi))
            if k < S - 1:
                zout[k + 1, g, 0] = low
                zout[k + 1, g, 1] = high
                send(k + 1, g, AXES)
            else:
                r = pl.ds(g * CG * XY, CG * XY)
                c = pltpu.make_async_copy(cur_v.at[r], out_h.at[r], out_sem.at[g])
                c.start()
                outs.append(c)
    for c in copies1 + copies2 + copies3:
        c.wait_send()
    for k in range(S):
        for g in range(G):
            wait_sends(k, g)
    for c in outs:
        c.wait()


def body(sizes, gradient, noise_draw, current, eigvectors, eigvalues, reaction):
    C, X, Y, Z = gradient.shape
    R = eigvectors.shape[3]
    NX, NY, NZ = sizes
    PL = NX * NY
    G = GROUPS
    CG = C // G
    S = SWEEPS - 1
    XY = X * Y
    f32, bf16 = jnp.float32, jnp.bfloat16
    rows = C * R // 128 // PL
    any_space = pl.BlockSpec(memory_space=pl.ANY)
    dma = pltpu.SemaphoreType.DMA
    out = pl.pallas_call(
        functools.partial(kernel, sizes, (C, X, Y, Z, R)),
        out_shape=jax.ShapeDtypeStruct((C * XY, Z), f32),
        in_specs=[any_space] * 4 + [pl.BlockSpec(memory_space=pltpu.VMEM), any_space],
        out_specs=any_space,
        scratch_shapes=[
            pltpu.VMEM((X, Y * Z, R), bf16),
            pltpu.VMEM((C * XY, Z), bf16),
            pltpu.VMEM((C * XY, Z), bf16),
            pltpu.VMEM((C * XY, Z), f32),
            pltpu.VMEM((C * XY, Z), f32),
            pltpu.VMEM((C * XY, Z), f32),
            pltpu.VMEM((X, Y, Z), f32),
            pltpu.VMEM((X, 2 * C, Y * Z), bf16),
            pltpu.VMEM((G, X, Y, CG, Z), f32),
            pltpu.VMEM((S, G, X + 2, Y + 2, CG, Z), f32),
            pltpu.VMEM((S, G, 2, CG, Z), f32),
            pltpu.VMEM((S, G, 2, CG, Z), f32),
            pltpu.VMEM((PL, rows, 128), f32),
            pltpu.VMEM((PL, rows, 128), f32),
            pltpu.VMEM((NZ, rows, 128), f32),
            pltpu.VMEM((PL, rows, 128), f32),
            dma((4 + X,)),
            dma((G,)),
            dma((PL,)), dma((PL,)),
            dma((NZ,)), dma((NZ,)),
            dma((PL,)), dma((PL,)),
            dma((S, G, 6)), dma((S, G, 6)),
        ],
        compiler_params=pltpu.CompilerParams(
            collective_id=0, has_side_effects=True, vmem_limit_bytes=67043328
        ),
    )(
        gradient.reshape(C * XY, Z),
        noise_draw.reshape(C * XY, Z),
        current.reshape(C * XY, Z),
        eigvectors.reshape(X, Y * Z, R),
        eigvalues.reshape(1, R),
        reaction,
    )
    return out.reshape(current.shape)


def solution(mesh):
    return jax.shard_map(
        functools.partial(body, tuple(mesh.shape[a] for a in AXES)),
        mesh=mesh,
        in_specs=(
            P(None, "gx", "gy", "gz"),
            P(None, "gx", "gy", "gz"),
            P(None, "gx", "gy", "gz"),
            P("gx", "gy", "gz", None),
            P(),
            P("gx", "gy", "gz"),
        ),
        out_specs=P(None, "gx", "gy", "gz"),
        check_vma=False,
    )
```
